32 devices in a mesh: dp: 2 (over x), sp: 4 (over z), cp: 4 (over y, core).
Axes of the slice: x: 2, y: 2, z: 4, core: 2. Of those that a mesh axis runs over, the one named last changes fastest.
Arguments:
- x_act: bfloat16 [48, 96, 28, 512], P('dp', 'sp', None, 'cp'), parts along dimension 0
- w_one: bfloat16 [3, 3, 512, 2048], P(None, None, 'cp')
- w_two: bfloat16 [3, 3, 2048, 512], P(None, None, 'cp')
- bias_one: float32 [2048], replicated
Outputs:
- output: bfloat16 [48, 96, 28, 512], P('dp', 'sp', None, 'cp'), parts along dimension 0
There are 2 independent parts. The reference program is written for one: setup_inputs(seed, part) draws one part's arguments, and reference() takes and returns one part's arrays. A program takes and returns all parts, laid end to end along the dimension named above; an argument that names none is the same for every part.
All inputs are finite; a program needn't handle non-finite values.
Results may differ from the reference program's by a relative error of at most 0.001.
Values are sent between devices in bfloat16 or wider.
A program may use at most 1 GiB of HBM per device.

```python
import jax
import jax.numpy as jnp
from jax import lax

BATCH_SIZE = 24
GRID_ROWS = 96
GRID_COLS = 28
CHANNELS = 512
HIDDEN_CHANNELS = 4 * CHANNELS
CONV_DIMS = ("NHWC", "HWIO", "NHWC")


def setup_inputs(seed: int = 0, part: int = 0) -> dict:
    base_key = jax.random.key(seed)
    key_x, key_one, key_two, key_bias = jax.random.split(base_key, 4)
    x_act = jax.random.normal(jax.random.fold_in(key_x, part), (BATCH_SIZE, GRID_ROWS, GRID_COLS, CHANNELS), jnp.float32)
    w_one = jax.random.normal(key_one, (3, 3, CHANNELS, HIDDEN_CHANNELS), jnp.float32) * (9 * CHANNELS) ** -0.5
    w_two = jax.random.normal(key_two, (3, 3, HIDDEN_CHANNELS, CHANNELS), jnp.float32) * (9 * HIDDEN_CHANNELS) ** -0.5
    bias_one = 0.7 * jax.random.normal(key_bias, (HIDDEN_CHANNELS,), jnp.float32)
    return {"x_act": x_act.astype(jnp.bfloat16), "w_one": w_one.astype(jnp.bfloat16), "w_two": w_two.astype(jnp.bfloat16), "bias_one": bias_one}


def reference(x_act, w_one, w_two, bias_one):
    w_first = w_one.astype(jnp.float32)
    w_second = w_two.astype(jnp.float32)

    def one_picture(picture):
        pic_f32 = picture.astype(jnp.float32)[None]
        pre_act = lax.conv_general_dilated(pic_f32, w_first, (1, 1), "SAME", dimension_numbers=CONV_DIMS)
        hidden = jax.nn.relu(pre_act + bias_one).astype(jnp.bfloat16)
        post_act = lax.conv_general_dilated(hidden.astype(jnp.float32), w_second, (1, 1), "SAME", dimension_numbers=CONV_DIMS)
        return (pic_f32 + post_act)[0].astype(jnp.bfloat16)

    return lax.map(one_picture, x_act)
```

```python
import jax
import jax.numpy as jnp
from jax import lax
from jax.sharding import PartitionSpec as P

CONV_DIMS = ("NHWC", "HWIO", "NHWC")
TAIL_ROWS = (4, 4, 4)


def solution(mesh):
    row_devs = mesh.shape["sp"]
    replicas = mesh.shape["dp"] * row_devs
    down_perm = [(d, d + 1) for d in range(row_devs - 1)]
    up_perm = [(d + 1, d) for d in range(row_devs - 1)]
    other_chip = [(i, i ^ 2) for i in range(4)]
    other_core = [(i, i ^ 1) for i in range(4)]
    other_corner = [(i, i ^ 3) for i in range(4)]
    act_spec = P("dp", "sp", None, "cp")
    kernel_spec = P(None, None, "cp", None)

    def swap_chip(v):
        return lax.ppermute(v, "cp", other_chip)

    def swap_core(v):
        return lax.ppermute(v, "cp", other_core)

    def conv_rows(padded, kernel):
        return lax.conv_general_dilated(padded, kernel, (1, 1), ((0, 0), (1, 1)), dimension_numbers=CONV_DIMS, preferred_element_type=jnp.float32)

    def pick(w, blocks, width):
        return jnp.concatenate([lax.dynamic_slice_in_dim(w, b * width, width, w.ndim - 1) for b in blocks], axis=-1)

    def local_block(x_tile, w_one_part, w_two_part, bias):
        place = lax.axis_index("cp")
        chip, core = place // 2, place % 2
        sp = lax.axis_index("sp")
        rows = x_tile.shape[1]
        half = rows // 2
        wide = w_two_part.shape[2]
        block = x_tile.shape[3]
        here, there = 2 * chip + core, 2 * (1 - chip) + core
        beside, across = 2 * chip + 1 - core, 2 * (1 - chip) + 1 - core
        replica = lax.axis_index("dp") * row_devs + sp

        def eighth(w):
            flat = w.reshape(-1, w.shape[-1])
            share = flat.shape[0] // replicas
            return lax.dynamic_slice_in_dim(flat, replica * share, share, 0)

        share_one = eighth(w_one_part)
        w1_part = swap_chip(pick(share_one, (there, here), wide))
        w1_part_beside = lax.ppermute(pick(share_one, (across, beside), wide), "cp", other_corner)
        w1_near_send = pick(w_one_part, (beside, across), wide)
        from_above = lax.ppermute(x_tile[:, -2:], "sp", down_perm)
        from_below = lax.ppermute(x_tile[:, :2], "sp", up_perm)
        upper, lower = x_tile[:, :half + 2], x_tile[:, half - 2:]
        far_inner = swap_chip(jnp.where(chip == 0, lower, upper))
        from_above, from_below, w1_part, w1_part_beside = lax.optimization_barrier((from_above, from_below, w1_part, w1_part_beside))
        w1_part = jnp.concatenate([w1_part, w1_part_beside], axis=0)
        w1_halves = [lax.all_gather(w1_part[:, i * wide:(i + 1) * wide], ("dp", "sp"), axis=0, tiled=True) for i in range(2)]

        x_mine = jnp.where(chip == 0, jnp.concatenate([from_above, upper], axis=1), jnp.concatenate([lower, from_below], axis=1))
        far_edge = swap_chip(jnp.where(chip == 0, from_below, from_above))
        w1_near = jnp.concatenate([pick(w_one_part, (here, there), wide), swap_core(w1_near_send)], axis=2)
        x_near = jnp.concatenate([x_mine, swap_core(x_mine)], axis=3)
        w2_part = swap_chip(pick(eighth(w_two_part), (across, beside, there, here), block))
        near_sum = conv_rows(x_near, w1_near)

        w1_halves[0], far_edge, far_inner, near_sum = lax.optimization_barrier((w1_halves[0], far_edge, far_inner, near_sum))
        x_far = jnp.where(chip == 0, jnp.concatenate([far_edge, far_inner], axis=1), jnp.concatenate([far_inner, far_edge], axis=1))
        share = w_one_part.shape[0] * w_one_part.shape[1] * block // replicas

        def far_kernel(both):
            own, beside_part = jnp.swapaxes(both.reshape(replicas, 2, share, wide), 0, 1).reshape(2, 3, 3, block, wide)
            return jnp.concatenate([own, beside_part], axis=2)

        bias_here = pick(bias, (here, there), wide)
        a_rows = lax.broadcasted_iota(jnp.int32, (1, half + 2, 1, 1), 1) + (rows * sp + half * chip - 1)
        inside = (a_rows >= 0) & (a_rows < rows * row_devs)
        x_far_all = jnp.concatenate([x_far, swap_core(x_far)], axis=3)

        def hidden_block(i):
            cols = slice(i * wide, (i + 1) * wide)
            summed = near_sum[..., cols] + conv_rows(x_far_all, far_kernel(w1_halves[i]))
            return jnp.where(inside, jax.nn.relu(summed + bias_here[cols]), 0.0).astype(jnp.bfloat16)

        hidden_here = hidden_block(0)
        w1_halves[1], w2_part, hidden_here = lax.optimization_barrier((w1_halves[1], w2_part, hidden_here))
        hidden = hidden_block(1)
        w2_far = lax.all_gather(w2_part, ("dp", "sp"), axis=0, tiled=True).reshape(w_two_part.shape)
        w2_near = pick(w_two_part, (beside, across, here, there), block)
        near_two = conv_rows(hidden_here, w2_near)
        hidden, w2_far, near_two = lax.optimization_barrier((hidden, w2_far, near_two))

        skip = jnp.concatenate([x_mine, x_far], axis=3)[:, 2:-2].astype(jnp.float32)
        spans, first = [], 0
        for length in TAIL_ROWS:
            spans.append((first, length))
            first += length

        def far_two(source, span, columns):
            return near_two[:, span[0]:span[0] + span[1], :, columns] + conv_rows(source[:, span[0]:span[0] + span[1] + 2], w2_far[..., columns])

        give_cols, keep_cols = slice(0, 2 * block), slice(2 * block, 4 * block)
        mine, back = [], []
        got = swap_core(far_two(hidden, spans[0], give_cols))
        for i, span in enumerate(spans):
            if i + 1 < len(spans):
                given = far_two(hidden, spans[i + 1], give_cols)
                hidden, given = lax.optimization_barrier((hidden, given))
                upcoming = swap_core(given)
            total = far_two(hidden, span, keep_cols)
            y_two = (skip[:, span[0]:span[0] + span[1]] + (total + got)).astype(jnp.bfloat16)
            if i + 1 < len(spans):
                hidden, y_two = lax.optimization_barrier((hidden, y_two))
                got = upcoming
            mine.append(y_two[..., :block])
            back.append(swap_chip(y_two[..., block:]))
        mine, back = jnp.concatenate(mine, axis=1), jnp.concatenate(back, axis=1)
        upper, lower = jnp.where(chip == 0, mine, back), jnp.where(chip == 0, back, mine)
        return jnp.concatenate([upper, lower], axis=1)

    return jax.shard_map(local_block, mesh=mesh, in_specs=(act_spec, kernel_spec, kernel_spec, P(None)), out_specs=act_spec, check_vma=False)
```

```python
import jax
import jax.numpy as jnp
from jax import lax
from jax.sharding import PartitionSpec as P


CONV_DIMS = ("NHWC", "HWIO", "NHWC")
TAIL_ROWS = (4, 4, 4)


def solution(mesh):
    row_devs = mesh.shape["sp"]
    replicas = mesh.shape["dp"] * row_devs
    down_perm = [(d, d + 1) for d in range(row_devs - 1)]
    up_perm = [(d + 1, d) for d in range(row_devs - 1)]
    other_chip = [(i, i ^ 2) for i in range(4)]
    other_core = [(i, i ^ 1) for i in range(4)]
    other_corner = [(i, i ^ 3) for i in range(4)]
    act_spec = P("dp", "sp", None, "cp")
    kernel_spec = P(None, None, "cp", None)

    def swap_chip(v):
        return lax.ppermute(v, "cp", other_chip)

    def swap_core(v):
        return lax.ppermute(v, "cp", other_core)

    def conv_rows(padded, kernel):
        return lax.conv_general_dilated(padded, kernel, (1, 1), ((0, 0), (1, 1)), dimension_numbers=CONV_DIMS, preferred_element_type=jnp.float32)

    def pick(w, blocks, width):
        return jnp.concatenate([lax.dynamic_slice_in_dim(w, b * width, width, w.ndim - 1) for b in blocks], axis=-1)

    def block_body(x_tile, w_one_part, w_two_part, bias):
        place = lax.axis_index("cp")
        chip, core = place // 2, place % 2
        sp = lax.axis_index("sp")
        rows = x_tile.shape[1]
        half = rows // 2
        wide = w_two_part.shape[2]
        block = x_tile.shape[3]
        here, there = 2 * chip + core, 2 * (1 - chip) + core
        beside, across = 2 * chip + 1 - core, 2 * (1 - chip) + 1 - core
        replica = lax.axis_index("dp") * row_devs + sp

        def eighth(w):
            flat = w.reshape(-1, w.shape[-1])
            share = flat.shape[0] // replicas
            return lax.dynamic_slice_in_dim(flat, replica * share, share, 0)

        share_one = eighth(w_one_part)
        w1_part = swap_chip(pick(share_one, (there, here), wide))
        w1_part_beside = lax.ppermute(pick(share_one, (across, beside), wide), "cp", other_corner)
        w1_near_send = pick(w_one_part, (beside, across), wide)
        from_above = lax.ppermute(x_tile[:, -2:], "sp", down_perm)
        from_below = lax.ppermute(x_tile[:, :2], "sp", up_perm)
        upper, lower = x_tile[:, :half + 2], x_tile[:, half - 2:]
        far_source, inner = jnp.where(chip == 0, lower, upper), jnp.where(chip == 0, upper, lower)
        from_above, from_below, w1_part, w1_part_beside, far_source, inner, w1_near_send = lax.optimization_barrier((from_above, from_below, w1_part, w1_part_beside, far_source, inner, w1_near_send))
        far_inner = swap_chip(far_source)
        w1_part = jnp.concatenate([w1_part, w1_part_beside], axis=0)
        w1_halves = []
        for i in range(2):
            w1_halves.append(lax.all_gather(w1_part[:, i * wide:(i + 1) * wide], ("dp", "sp"), axis=0, tiled=True))

        x_mine = jnp.where(chip == 0, jnp.concatenate([from_above, inner], axis=1), jnp.concatenate([inner, from_below], axis=1))
        far_edge = swap_chip(jnp.where(chip == 0, from_below, from_above))
        w1_near = jnp.concatenate([pick(w_one_part, (here, there), wide), swap_core(w1_near_send)], axis=2)
        x_near = jnp.concatenate([x_mine, swap_core(x_mine)], axis=3)
        w2_part = swap_chip(pick(eighth(w_two_part), (across, beside, there, here), block))
        near_sum = conv_rows(x_near, w1_near)

        w1_halves[0], far_edge, far_inner, near_sum = lax.optimization_barrier((w1_halves[0], far_edge, far_inner, near_sum))
        x_far = jnp.where(chip == 0, jnp.concatenate([far_edge, far_inner], axis=1), jnp.concatenate([far_inner, far_edge], axis=1))
        share = w_one_part.shape[0] * w_one_part.shape[1] * block // replicas

        def far_kernel(both):
            own, beside_part = jnp.swapaxes(both.reshape(replicas, 2, share, wide), 0, 1).reshape(2, 3, 3, block, wide)
            return jnp.concatenate([own, beside_part], axis=2)

        bias_here = pick(bias, (here, there), wide)
        a_rows = lax.broadcasted_iota(jnp.int32, (1, half + 2, 1, 1), 1) + (rows * sp + half * chip - 1)
        inside = (a_rows >= 0) & (a_rows < rows * row_devs)
        x_far_all = jnp.concatenate([x_far, swap_core(x_far)], axis=3)

        def hidden_block(i):
            cols = slice(i * wide, (i + 1) * wide)
            summed = near_sum[..., cols] + conv_rows(x_far_all, far_kernel(w1_halves[i]))
            return jnp.where(inside, jax.nn.relu(summed + bias_here[cols]), 0.0).astype(jnp.bfloat16)

        hidden_here = hidden_block(0)
        w1_halves[1], w2_part, hidden_here = lax.optimization_barrier((w1_halves[1], w2_part, hidden_here))
        hidden = hidden_block(1)
        w2_far = lax.all_gather(w2_part, ("dp", "sp"), axis=0, tiled=True).reshape(w_two_part.shape)
        w2_near = pick(w_two_part, (beside, across, here, there), block)
        near_two = conv_rows(hidden_here, w2_near)
        hidden, w2_far, near_two = lax.optimization_barrier((hidden, w2_far, near_two))

        skip = jnp.concatenate([x_mine, x_far], axis=3)[:, 2:-2].astype(jnp.float32)
        spans, first = [], 0
        for length in TAIL_ROWS:
            spans.append((first, length))
            first += length

        def far_two(source, span, columns):
            return near_two[:, span[0]:span[0] + span[1], :, columns] + conv_rows(source[:, span[0]:span[0] + span[1] + 2], w2_far[..., columns])

        give_cols, keep_cols = slice(0, 2 * block), slice(2 * block, 4 * block)
        mine, back = [], []
        got = swap_core(far_two(hidden, spans[0], give_cols))
        for i, span in enumerate(spans):
            if i + 1 < len(spans):
                given = far_two(hidden, spans[i + 1], give_cols)
                hidden, given = lax.optimization_barrier((hidden, given))
                upcoming = swap_core(given)
            total = far_two(hidden, span, keep_cols)
            y_two = (skip[:, span[0]:span[0] + span[1]] + (total + got)).astype(jnp.bfloat16)
            if i + 1 < len(spans):
                hidden, y_two = lax.optimization_barrier((hidden, y_two))
                got = upcoming
            mine.append(y_two[..., :block])
            back.append(swap_chip(y_two[..., block:]))
        mine, back = jnp.concatenate(mine, axis=1), jnp.concatenate(back, axis=1)
        upper, lower = jnp.where(chip == 0, mine, back), jnp.where(chip == 0, back, mine)
        return jnp.concatenate([upper, lower], axis=1)

    return jax.shard_map(block_body, mesh=mesh, in_specs=(act_spec, kernel_spec, kernel_spec, P(None)), out_specs=act_spec, check_vma=False)
```
